512 devices in a mesh: expert: 8 (over x, core), dp: 64 (over z, y).
Axes of the slice: x: 4, y: 8, z: 8, core: 2. Of those that a mesh axis runs over, the one named last changes fastest.
Arguments:
- tokens: bfloat16 [4096, 4096], P(('expert', 'dp')), may hold values from -6 to 6
- expert_ids: int32 [4096, 2], P(('expert', 'dp')), may hold values from 0 to 7, as said below
- slots: int32 [4096, 2], P(('expert', 'dp')), may hold values from -1 to 1, as said below
- mix_weights: float32 [4096, 2], P(('expert', 'dp')), may hold values from 0.1 to 1
- w_gate: bfloat16 [8, 4096, 8192], P('expert', None, 'dp'), may hold values from -0.09375 to 0.09375
- w_up: bfloat16 [8, 4096, 8192], P('expert', None, 'dp'), may hold values from -0.09375 to 0.09375
- w_down: bfloat16 [8, 8192, 4096], P('expert', None, 'dp'), may hold values from -0.0625 to 0.0625
Outputs:
- mixed: bfloat16 [4096, 4096], P(('expert', 'dp'))
The draws below stay inside these ranges and needn't reach their ends.
Inputs may be any that keep to these rules, and one draw needn't show every extreme that they name: `expert_ids`: each token names 2 different experts. Within each aligned block of 8 tokens (the tokens of one device), the assignments to one expert get distinct slots among 0 to 1 in some order, at most 2 of them are kept and the others get -1; an expert with 2 or more assignments in the block has all 2 slots used. No two assignments of one block share an expert and a slot. In every block some expert has all 2 slots used.
All inputs are finite; a program needn't handle non-finite values.
Results may differ from the reference program's by a relative error of at most 0.0085.
Values may be sent and summed in bfloat16 or wider, within the bound.
No kernel may reach another device: no remote copies, remote signals or barrier semaphores. Data moves between devices by JAX's collectives and lax.ppermute only.
A program may use at most 128 MiB of HBM per device.

```python
import jax
import jax.numpy as jnp
from jax import lax

D = 4096
FFW = 8192
TOP = 2
TOK_DEV = 8
CAP = 2
EXPERTS = 8
TOKENS = 4096
N_DP = 64


def routing(key):
    folded = jax.random.fold_in(key, 17)
    jitter_key, lean_key, favour_key, order_key = jax.random.split(folded, 4)
    jitter = jax.random.randint(jitter_key, (TOKENS, EXPERTS), 0, 2 ** 20)
    lean_bias = jax.random.randint(lean_key, (EXPERTS,), 0, 4) * 2 ** 19
    favoured = jax.random.randint(favour_key, (N_DP,), 0, EXPERTS)
    block_id = jnp.arange(TOKENS, dtype=jnp.int32) // TOK_DEV
    position = jnp.arange(TOKENS, dtype=jnp.int32) % TOK_DEV
    favoured_tok = favoured[block_id % N_DP]
    expert_line = jnp.arange(EXPERTS, dtype=jnp.int32)
    booster = ((position < CAP)[:, None] & (expert_line[None, :] == favoured_tok[:, None])).astype(jnp.int32) * 2 ** 23
    scores = (jitter + lean_bias[None, :] + booster) * EXPERTS + expert_line[None, :]
    top_scores, chosen = lax.top_k(scores, TOP)
    chosen = chosen.astype(jnp.int32)
    grouped = chosen.reshape(TOKENS // TOK_DEV, TOK_DEV * TOP)
    same_expert = grouped[:, :, None] == grouped[:, None, :]
    order_line = jnp.arange(TOK_DEV * TOP, dtype=jnp.int32)
    priority = jax.random.randint(order_key, (TOKENS // TOK_DEV, TOK_DEV * TOP), 0, 2 ** 16) * (TOK_DEV * TOP) + order_line[None, :]
    earlier = priority[:, None, :] < priority[:, :, None]
    position_rank = jnp.sum((same_expert & earlier).astype(jnp.int32), axis=2)
    slot_values = jnp.where(position_rank < CAP, position_rank, -1).astype(jnp.int32)
    return (chosen, slot_values.reshape(TOKENS, TOP))


def draw_expert_ids(key, part):
    return routing(key)[0]


def draw_slots(key, part):
    return routing(key)[1]


def levels(own_key, extent, cuts, least, largest):
    factor_of = 1.0
    for dim, parts in cuts:
        heights = jax.random.uniform(jax.random.fold_in(jax.random.fold_in(own_key, 6), dim), (parts,), jnp.float32, least / len(cuts), largest / len(cuts))
        factor_of = factor_of * jnp.repeat(jnp.exp(heights), extent[dim] // parts).reshape((-1,) + (1,) * (len(extent) - 1 - dim))
    return factor_of


def noise(own_key, shape, scale, most, cuts=(), held_as=jnp.bfloat16):
    level = levels(own_key, shape, cuts, -0.22, 0.18) if cuts else 1.0
    values = jax.random.normal(own_key, shape, jnp.float32) * scale * level
    return jnp.minimum(jnp.maximum(values, -most), most).astype(held_as)


def setup_inputs(seed: int = 0) -> dict:
    splits = jax.random.split(jax.random.key(seed), 8)
    tokens = noise(splits[0], (TOKENS, D), 1.0, 6.0, ((0, 512),))
    expert_ids = draw_expert_ids(jax.random.fold_in(splits[7], 71), 0)
    slots = draw_slots(jax.random.fold_in(splits[7], 71), 0)
    mix_weights = jnp.clip(0.1 + 0.9 * jax.random.uniform(splits[3], (TOKENS, TOP), jnp.float32) ** levels(splits[3], (TOKENS, TOP), ((0, 512),), -0.2, 0.2), 0.1, 1.0)
    w_gate = noise(splits[4], (EXPERTS, D, FFW), D ** -0.5, 0.09375, ((0, 8), (2, 64)))
    w_up = noise(splits[5], (EXPERTS, D, FFW), D ** -0.5, 0.09375, ((0, 8), (2, 64)))
    w_down = noise(splits[6], (EXPERTS, FFW, D), FFW ** -0.5, 0.0625, ((0, 8), (2, 64)))
    return dict(tokens=tokens, expert_ids=expert_ids, slots=slots, mix_weights=mix_weights, w_gate=w_gate, w_up=w_up, w_down=w_down)


def reference(tokens, expert_ids, slots, mix_weights, w_gate, w_up, w_down):
    block_count = TOKENS // TOK_DEV
    block_of = jnp.arange(TOKENS, dtype=jnp.int32) // TOK_DEV
    block_idx = jnp.broadcast_to(block_of[:, None], (TOKENS, TOP)).astype(jnp.int32)
    is_kept = slots >= 0
    slot_place = jnp.where(is_kept, slots, CAP).astype(jnp.int32)
    spread = jnp.broadcast_to(tokens[:, None, :], (TOKENS, TOP, D))
    buffer = jnp.zeros((EXPERTS, block_count, CAP, D), jnp.bfloat16)
    buffer = buffer.at[expert_ids, block_idx, slot_place].set(spread, mode="drop")

    def expert_ffn(operands):
        slab, gate_w, up_w, down_w = operands
        flattened = slab.reshape(block_count * CAP, D)
        gate_part = jnp.dot(flattened, gate_w, preferred_element_type=jnp.float32)
        up_part = jnp.dot(flattened, up_w, preferred_element_type=jnp.float32)
        hidden = (jax.nn.silu(gate_part) * up_part).astype(jnp.bfloat16)
        result = jnp.dot(hidden, down_w, preferred_element_type=jnp.float32).astype(jnp.bfloat16)
        return result.reshape(block_count, CAP, D)

    outputs = lax.map(expert_ffn, (buffer, w_gate, w_up, w_down))
    picked = outputs[expert_ids, block_idx, jnp.minimum(slot_place, CAP - 1)]
    weighted = jnp.where(is_kept[:, :, None], mix_weights[:, :, None] * picked.astype(jnp.float32), 0.0)
    return jnp.sum(weighted, axis=1).astype(jnp.bfloat16)
```

```python
import jax
import jax.numpy as jnp
from jax import lax
from jax.sharding import Mesh, PartitionSpec as P

CAP = 2
LANES = 128
STEPS = (64, 32, 16, 8)
GROUP = ("x", "core")
PLANE = ("z", "y")


def raise_rows(peak):
    k = jnp.zeros_like(peak)
    for p in STEPS:
        low = peak < 2.0 ** (15 - p)
        peak = jnp.where(low, peak * 2.0**p, peak)
        k = jnp.where(low, k + p, k)
    return k


def power(k, sign):
    out = jnp.ones_like(k)
    for p in STEPS:
        low = k >= p
        out = jnp.where(low, out * 2.0 ** (sign * p), out)
        k = jnp.where(low, k - p, k)
    return out


def shards(tokens, expert_ids, slots, mix_weights, w_gate, w_up, w_down):
    tok_rows, width = tokens.shape
    experts = lax.axis_size(GROUP)
    nz, ny = lax.axis_size("z"), lax.axis_size("y")
    slot_count = experts * CAP
    rows = nz * ny * slot_count
    unit = w_gate.shape[2]
    cols = w_down.shape[2]

    wd = w_down[0].T.reshape(cols, nz, ny, unit).transpose(2, 0, 1, 3)
    wd = lax.all_to_all(wd, "y", split_axis=0, concat_axis=0, tiled=True)
    wd = wd.reshape(ny * cols, nz * unit)

    slot_ids = jnp.arange(slot_count, dtype=jnp.int32)
    matches = (expert_ids[None, :, :] == (slot_ids // CAP)[:, None, None]) & (
        slots[None, :, :] == (slot_ids % CAP)[:, None, None]
    )
    table = jnp.any(matches, axis=2).astype(jnp.bfloat16)
    wide = tokens.astype(jnp.float32)
    k = raise_rows(jnp.max(jnp.abs(wide), axis=1, keepdims=True))
    lifted = (wide * power(k, 1)).astype(jnp.bfloat16)
    held = jnp.concatenate(
        [lifted, jnp.broadcast_to(k, (tok_rows, LANES)).astype(jnp.bfloat16)], axis=1
    )
    outgoing = jnp.dot(table, held, preferred_element_type=jnp.float32).astype(jnp.float16)
    arrived = lax.all_to_all(outgoing, GROUP, split_axis=0, concat_axis=0, tiled=True)
    portion = lax.all_gather(arrived, PLANE, axis=0, tiled=True)
    x = portion[:, :width].astype(jnp.bfloat16)
    lower = power(portion[:, width : width + 1].astype(jnp.float32), -1)

    gate = jnp.dot(x, w_gate[0], preferred_element_type=jnp.float32) * lower
    up = jnp.dot(x, w_up[0], preferred_element_type=jnp.float32) * lower
    hidden = jax.nn.silu(gate) * up
    hidden = hidden * 2.0**-8
    hk = raise_rows(jnp.max(jnp.abs(hidden), axis=1))
    packed = (hidden * power(hk, 1)[:, None]).astype(jnp.float16)
    packed = jnp.concatenate([packed, hk.reshape(rows // LANES, LANES).astype(jnp.float16)], axis=0)
    spread = lax.all_gather(packed, "z", axis=0, tiled=False)
    drop = power(spread[:, rows:].astype(jnp.float32).reshape(nz, rows), -1) * 2.0**8
    h = (spread[:, :rows].astype(jnp.float32) * drop[:, :, None]).astype(jnp.bfloat16)
    h = h.transpose(1, 0, 2).reshape(rows, nz * unit)
    part = lax.dot_general(
        h, wd, (((1,), (1,)), ((), ())), preferred_element_type=jnp.float32
    ).astype(jnp.bfloat16)
    part = part.reshape(nz * ny, slot_count, ny * cols)
    part = lax.all_to_all(part, PLANE, split_axis=0, concat_axis=0, tiled=True)
    part = part.reshape(nz, ny, slot_count, ny * cols).astype(jnp.float32).sum(axis=1)
    result = part.transpose(1, 0, 2).reshape(slot_count, width).astype(jnp.bfloat16)
    back = lax.all_to_all(result, GROUP, split_axis=0, concat_axis=0, tiled=True)
    weights = jnp.sum(jnp.where(matches, mix_weights[None, :, :], 0.0), axis=2)
    mixed = jnp.dot(weights.T, back.astype(jnp.float32), preferred_element_type=jnp.float32)
    return mixed.astype(jnp.bfloat16)


def solution(mesh):
    experts, dp = mesh.devices.shape
    ny = 8 if dp % 8 == 0 else 1
    split = Mesh(
        mesh.devices.reshape(experts // 2, 2, dp // ny, ny), ("x", "core", "z", "y")
    )
    tok = P(GROUP + PLANE, None)
    weight = P(GROUP, None, PLANE)
    return jax.shard_map(
        shards,
        mesh=split,
        in_specs=(tok, tok, tok, tok, weight, weight, weight),
        out_specs=tok,
        check_vma=False,
    )
```

```python
import jax
import jax.numpy as jnp
from jax import lax
from jax.experimental import pallas as pl
from jax.experimental.pallas import tpu as pltpu
from jax.sharding import Mesh, PartitionSpec as P

CAP = 2
BLOCK = 256
LANES = 128
STEPS = (64, 32, 16, 8)
GROUP = ("x", "core")
PLANE = ("z", "y")


def raise_rows(peak):
    k = jnp.zeros_like(peak)
    for p in STEPS:
        low = peak < 2.0 ** (15 - p)
        peak = jnp.where(low, peak * 2.0**p, peak)
        k = jnp.where(low, k + p, k)
    return k


def power(k, sign):
    out = jnp.ones_like(k)
    for p in STEPS:
        low = k >= p
        out = jnp.where(low, out * 2.0 ** (sign * p), out)
        k = jnp.where(low, k - p, k)
    return out


def down_kernel(h_ref, w_ref, o_ref, w_all):
    nz, rows, unit = h_ref.shape
    ny, _, cols, _ = w_ref.shape
    for z in range(nz):
        for y in range(ny):
            w_all[pl.ds(y * cols, cols), pl.ds(z * unit, unit)] = w_ref[y, z]

    @pl.loop(0, rows // BLOCK)
    def _(i):
        at = pl.ds(pl.multiple_of(i * BLOCK, BLOCK), BLOCK)
        h = jnp.concatenate([h_ref[z, at, :] for z in range(nz)], axis=1)
        o_ref[at, :] = lax.dot_general(
            h, w_all[...], (((1,), (1,)), ((), ())), preferred_element_type=jnp.float32
        ).astype(o_ref.dtype)


def down(h, w):
    nz, rows, unit = h.shape
    ny, _, cols, _ = w.shape
    return pl.pallas_call(
        down_kernel,
        out_shape=jax.ShapeDtypeStruct((rows, ny * cols), jnp.bfloat16),
        in_specs=[pl.BlockSpec(memory_space=pltpu.VMEM)] * 2,
        out_specs=pl.BlockSpec(memory_space=pltpu.VMEM),
        compiler_params=pltpu.CompilerParams(vmem_limit_bytes=16 << 20),
        scratch_shapes=[pltpu.VMEM((ny * cols, nz * unit), jnp.bfloat16)],
        cost_estimate=pl.CostEstimate(
            flops=2 * rows * nz * unit * ny * cols, bytes_accessed=4 << 20, transcendentals=0
        ),
    )(h, w)


def shards(tokens, expert_ids, slots, mix_weights, w_gate, w_up, w_down):
    tok_rows, width = tokens.shape
    experts = lax.axis_size(GROUP)
    nz, ny = lax.axis_size("z"), lax.axis_size("y")
    slot_count = experts * CAP
    unit = w_gate.shape[2]
    cols = w_down.shape[2]

    wd = w_down[0].T.reshape(cols, nz, ny, unit).transpose(2, 1, 0, 3)

    slot_ids = jnp.arange(slot_count, dtype=jnp.int32)
    matches = (expert_ids[None, :, :] == (slot_ids // CAP)[:, None, None]) & (
        slots[None, :, :] == (slot_ids % CAP)[:, None, None]
    )
    table = jnp.any(matches, axis=2).astype(jnp.bfloat16)
    wide = tokens.astype(jnp.float32)
    k = raise_rows(jnp.max(jnp.abs(wide), axis=1, keepdims=True))
    lifted = (wide * power(k, 1)).astype(jnp.bfloat16)
    held = jnp.concatenate(
        [lifted, jnp.broadcast_to(k, (tok_rows, LANES)).astype(jnp.bfloat16)], axis=1
    )
    outgoing = jnp.dot(table, held, preferred_element_type=jnp.float32).astype(jnp.float16)
    arrived = lax.all_to_all(outgoing, GROUP, split_axis=0, concat_axis=0, tiled=True)
    portion = lax.all_gather(arrived, PLANE, axis=0, tiled=True)
    x = portion[:, :width].astype(jnp.bfloat16)
    lower = power(portion[:, width : width + 1].astype(jnp.float32), -1)

    gate = jnp.dot(x, w_gate[0], preferred_element_type=jnp.float32) * lower
    up = jnp.dot(x, w_up[0], preferred_element_type=jnp.float32) * lower
    hidden = jax.nn.silu(gate) * up
    packed = jnp.sqrt(jnp.sqrt(jnp.abs(hidden * 2.0**40)))
    packed = jnp.where(hidden < 0, -packed, packed).astype(jnp.float16)
    packed, wd = lax.optimization_barrier((packed, wd))
    wd = lax.all_to_all(wd, "y", split_axis=0, concat_axis=0, tiled=True)
    spread = lax.all_gather(packed, "z", axis=0, tiled=False)
    spread = spread.astype(jnp.float32)
    h = (spread * jnp.abs(spread) * (spread * spread * 2.0**-40)).astype(jnp.bfloat16)
    part = down(h, wd)
    part = part.reshape(nz * ny, slot_count, ny * cols)
    part = lax.all_to_all(part, PLANE, split_axis=0, concat_axis=0, tiled=True)
    part = part.reshape(nz, ny, slot_count, ny * cols).astype(jnp.float32).sum(axis=1)
    result = part.transpose(1, 0, 2).reshape(slot_count, width).astype(jnp.bfloat16)
    back = lax.all_to_all(result, GROUP, split_axis=0, concat_axis=0, tiled=True)
    weights = jnp.sum(jnp.where(matches, mix_weights[None, :, :], 0.0), axis=2)
    mixed = jnp.dot(weights.T, back.astype(jnp.float32), preferred_element_type=jnp.float32)
    return mixed.astype(jnp.bfloat16)


def solution(mesh):
    experts, dp = mesh.devices.shape
    ny = 8 if dp % 8 == 0 else 1
    split = Mesh(
        mesh.devices.reshape(experts // 2, 2, dp // ny, ny), ("x", "core", "z", "y")
    )
    tok = P(GROUP + PLANE, None)
    weight = P(GROUP, None, PLANE)
    return jax.shard_map(
        shards,
        mesh=split,
        in_specs=(tok, tok, tok, tok, weight, weight, weight),
        out_specs=tok,
        check_vma=False,
    )
```

```python
import jax
import jax.numpy as jnp
from jax import lax
from jax.experimental import pallas as pl
from jax.experimental.pallas import tpu as pltpu
from jax.sharding import Mesh, PartitionSpec as P

CAP = 2
BLOCK = 256
GROUP = ("x", "core")
PLANE = ("z", "y")


def down_kernel(h_ref, w_ref, o_ref, w_all):
    nz, rows, unit = h_ref.shape
    ny, _, cols, _ = w_ref.shape
    for z in range(nz):
        for y in range(ny):
            w_all[pl.ds(y * cols, cols), pl.ds(z * unit, unit)] = w_ref[y, z]

    @pl.loop(0, rows // BLOCK)
    def _(i):
        at = pl.ds(pl.multiple_of(i * BLOCK, BLOCK), BLOCK)
        h = jnp.concatenate([h_ref[z, at, :] for z in range(nz)], axis=1)
        o_ref[at, :] = lax.dot_general(
            h, w_all[...], (((1,), (1,)), ((), ())), preferred_element_type=jnp.float32
        ).astype(o_ref.dtype)


def down(h, w):
    nz, rows, unit = h.shape
    ny, _, cols, _ = w.shape
    return pl.pallas_call(
        down_kernel,
        out_shape=jax.ShapeDtypeStruct((rows, ny * cols), jnp.bfloat16),
        in_specs=[pl.BlockSpec(memory_space=pltpu.VMEM)] * 2,
        out_specs=pl.BlockSpec(memory_space=pltpu.VMEM),
        compiler_params=pltpu.CompilerParams(vmem_limit_bytes=16 << 20),
        scratch_shapes=[pltpu.VMEM((ny * cols, nz * unit), jnp.bfloat16)],
        cost_estimate=pl.CostEstimate(
            flops=2 * rows * nz * unit * ny * cols, bytes_accessed=4 << 20, transcendentals=0
        ),
    )(h, w)


def shards(tokens, expert_ids, slots, mix_weights, w_gate, w_up, w_down):
    _, width = tokens.shape
    experts = lax.axis_size(GROUP)
    nz, ny = lax.axis_size("z"), lax.axis_size("y")
    slot_count = experts * CAP
    unit = w_gate.shape[2]
    cols = w_down.shape[2]

    wd = w_down[0].T.reshape(cols, nz, ny, unit).transpose(2, 1, 0, 3)

    slot_ids = jnp.arange(slot_count, dtype=jnp.int32)
    matches = (expert_ids[None, :, :] == (slot_ids // CAP)[:, None, None]) & (
        slots[None, :, :] == (slot_ids % CAP)[:, None, None]
    )
    table = jnp.any(matches, axis=2).astype(jnp.bfloat16)
    outgoing = jnp.dot(table, tokens, preferred_element_type=jnp.float32)
    root = jnp.sqrt(jnp.abs(outgoing * 2.0**29))
    outgoing = jnp.where(outgoing < 0, -root, root).astype(jnp.float16)
    arrived = lax.all_to_all(outgoing, GROUP, split_axis=0, concat_axis=0, tiled=True)
    portion = lax.all_gather(arrived, PLANE, axis=0, tiled=True)
    root = portion.astype(jnp.float32)
    x = (root * jnp.abs(root)).astype(jnp.bfloat16)
    gate = jnp.dot(x, w_gate[0], preferred_element_type=jnp.float32) * 2.0**-29
    up = jnp.dot(x, w_up[0], preferred_element_type=jnp.float32) * 2.0**-29
    hidden = jax.nn.silu(gate) * up
    packed = jnp.sqrt(jnp.sqrt(jnp.abs(hidden * 2.0**40)))
    packed = jnp.where(hidden < 0, -packed, packed).astype(jnp.float16)
    packed, wd = lax.optimization_barrier((packed, wd))
    wd = lax.all_to_all(wd, "y", split_axis=0, concat_axis=0, tiled=True)
    spread = lax.all_gather(packed, "z", axis=0, tiled=False)
    spread = spread.astype(jnp.float32)
    h = (spread * jnp.abs(spread) * (spread * spread * 2.0**-40)).astype(jnp.bfloat16)
    part = down(h, wd)
    part = part.reshape(nz * ny, slot_count, ny * cols)
    part = lax.all_to_all(part, PLANE, split_axis=0, concat_axis=0, tiled=True)
    part = part.reshape(nz, ny, slot_count, ny * cols).astype(jnp.float32).sum(axis=1)
    result = part.transpose(1, 0, 2).reshape(slot_count, width).astype(jnp.bfloat16)
    back = lax.all_to_all(result, GROUP, split_axis=0, concat_axis=0, tiled=True)
    weights = jnp.sum(jnp.where(matches, mix_weights[None, :, :], 0.0), axis=2)
    mixed = jnp.dot(weights.T, back.astype(jnp.float32), preferred_element_type=jnp.float32)
    return mixed.astype(jnp.bfloat16)


def solution(mesh):
    experts, dp = mesh.devices.shape
    ny = 8 if dp % 8 == 0 else 1
    split = Mesh(
        mesh.devices.reshape(experts // 2, 2, dp // ny, ny), ("x", "core", "z", "y")
    )
    tok = P(GROUP + PLANE, None)
    weight = P(GROUP, None, PLANE)
    return jax.shard_map(
        shards,
        mesh=split,
        in_specs=(tok, tok, tok, tok, weight, weight, weight),
        out_specs=tok,
        check_vma=False,
    )
```

```python
import jax
import jax.numpy as jnp
from jax import lax
from jax.experimental import pallas as pl
from jax.experimental.pallas import tpu as pltpu
from jax.sharding import Mesh, PartitionSpec as P

CAP = 2
GROUP = ("x", "core")
PLANE = ("z", "y")


def down_kernel(h_ref, w_ref, o_ref, w_all):
    nz, _, unit = h_ref.shape
    ny, _, cols, _ = w_ref.shape
    for z in range(nz):
        for y in range(ny):
            w_all[pl.ds(y * cols, cols), pl.ds(z * unit, unit)] = w_ref[y, z]

    h = jnp.concatenate([h_ref[z] for z in range(nz)], axis=1)
    o_ref[...] = lax.dot_general(
        h, w_all[...], (((1,), (1,)), ((), ())), preferred_element_type=jnp.float32
    ).astype(o_ref.dtype)


def down(h, w):
    nz, rows, unit = h.shape
    ny, _, cols, _ = w.shape
    return pl.pallas_call(
        down_kernel,
        out_shape=jax.ShapeDtypeStruct((rows, ny * cols), jnp.bfloat16),
        in_specs=[pl.BlockSpec(memory_space=pltpu.VMEM)] * 2,
        out_specs=pl.BlockSpec(memory_space=pltpu.VMEM),
        compiler_params=pltpu.CompilerParams(vmem_limit_bytes=20 << 20),
        scratch_shapes=[pltpu.VMEM((ny * cols, nz * unit), jnp.bfloat16)],
        cost_estimate=pl.CostEstimate(
            flops=2 * rows * nz * unit * ny * cols, bytes_accessed=4 << 20, transcendentals=0
        ),
    )(h, w)


def shards(tokens, expert_ids, slots, mix_weights, w_gate, w_up, w_down):
    _, width = tokens.shape
    experts = lax.axis_size(GROUP)
    nz, ny = lax.axis_size("z"), lax.axis_size("y")
    slot_count = experts * CAP
    unit = w_gate.shape[2]
    cols = w_down.shape[2]

    wd = w_down[0].T.reshape(cols, nz, ny, unit).transpose(2, 1, 0, 3)

    pair = jnp.concatenate([w_gate[0], w_up[0]], axis=1)

    slot_ids = jnp.arange(slot_count, dtype=jnp.int32)
    matches = (expert_ids[None, :, :] == (slot_ids // CAP)[:, None, None]) & (
        slots[None, :, :] == (slot_ids % CAP)[:, None, None]
    )
    table = jnp.any(matches, axis=2).astype(jnp.bfloat16)
    outgoing = jnp.dot(table, tokens, preferred_element_type=jnp.float32)
    root = jnp.sqrt(jnp.abs(outgoing * 2.0**29))
    outgoing = jnp.where(outgoing < 0, -root, root).astype(jnp.float16)
    arrived = lax.all_to_all(outgoing, GROUP, split_axis=0, concat_axis=0, tiled=True)
    portion = lax.all_gather(arrived, PLANE, axis=0, tiled=True)
    root = portion.astype(jnp.float32)
    x = (root * jnp.abs(root)).astype(jnp.bfloat16)
    both = jnp.dot(x, pair, preferred_element_type=jnp.float32) * 2.0**-29
    gate, up = both[:, :unit], both[:, unit:]
    hidden = jax.nn.silu(gate) * up
    packed = jnp.sqrt(jnp.sqrt(jnp.abs(hidden * 2.0**40)))
    packed = jnp.where(hidden < 0, -packed, packed).astype(jnp.float16)
    packed, wd = lax.optimization_barrier((packed, wd))
    wd = lax.all_to_all(wd, "y", split_axis=0, concat_axis=0, tiled=True)
    spread = lax.all_gather(packed, "z", axis=0, tiled=False)
    spread = spread.astype(jnp.float32)
    h = (spread * jnp.abs(spread) * (spread * spread * 2.0**-40)).astype(jnp.bfloat16)
    part = down(h, wd)
    part = part.reshape(nz * ny, slot_count, ny * cols)
    part = lax.all_to_all(part, PLANE, split_axis=0, concat_axis=0, tiled=True)
    part = part.reshape(nz, ny, slot_count, ny * cols).astype(jnp.float32).sum(axis=1)
    result = part.transpose(1, 0, 2).reshape(slot_count, width).astype(jnp.bfloat16)
    back = lax.all_to_all(result, GROUP, split_axis=0, concat_axis=0, tiled=True)
    weights = jnp.sum(jnp.where(matches, mix_weights[None, :, :], 0.0), axis=2)
    mixed = jnp.dot(weights.T, back.astype(jnp.float32), preferred_element_type=jnp.float32)
    return mixed.astype(jnp.bfloat16)


def solution(mesh):
    experts, dp = mesh.devices.shape
    ny = 8 if dp % 8 == 0 else 1
    split = Mesh(
        mesh.devices.reshape(experts // 2, 2, dp // ny, ny), ("x", "core", "z", "y")
    )
    tok = P(GROUP + PLANE, None)
    weight = P(GROUP, None, PLANE)
    return jax.shard_map(
        shards,
        mesh=split,
        in_specs=(tok, tok, tok, tok, weight, weight, weight),
        out_specs=tok,
        check_vma=False,
    )
```

```python
import jax
import jax.numpy as jnp
from jax import lax
from jax.experimental import pallas as pl
from jax.experimental.pallas import tpu as pltpu
from jax.sharding import Mesh, PartitionSpec as P

CAP = 2
GROUP = ("x", "core")
PLANE = ("z", "y")


def down_kernel(h_ref, w_ref, o_ref, w_all):
    nz, _, unit = h_ref.shape
    ny, _, cols, _ = w_ref.shape
    for z in range(nz):
        for y in range(ny):
            w_all[pl.ds(y * cols, cols), pl.ds(z * unit, unit)] = w_ref[y, z]

    h = jnp.concatenate([h_ref[z] for z in range(nz)], axis=1)
    o_ref[...] = lax.dot_general(
        h, w_all[...], (((1,), (1,)), ((), ())), preferred_element_type=jnp.float32
    ).astype(o_ref.dtype)


def down(h, w):
    nz, rows, unit = h.shape
    ny, _, cols, _ = w.shape
    return pl.pallas_call(
        down_kernel,
        out_shape=jax.ShapeDtypeStruct((rows, ny * cols), jnp.bfloat16),
        in_specs=[pl.BlockSpec(memory_space=pltpu.VMEM)] * 2,
        out_specs=pl.BlockSpec(memory_space=pltpu.VMEM),
        compiler_params=pltpu.CompilerParams(vmem_limit_bytes=20 << 20),
        scratch_shapes=[pltpu.VMEM((ny * cols, nz * unit), jnp.bfloat16)],
        cost_estimate=pl.CostEstimate(
            flops=2 * rows * nz * unit * ny * cols, bytes_accessed=4 << 20, transcendentals=0
        ),
    )(h, w)


def shards(tokens, expert_ids, slots, mix_weights, w_gate, w_up, w_down):
    _, width = tokens.shape
    experts = lax.axis_size(GROUP)
    nz, ny = lax.axis_size("z"), lax.axis_size("y")
    slot_count = experts * CAP
    rows = nz * ny * slot_count
    unit = w_gate.shape[2]
    cols = w_down.shape[2]

    wd = w_down[0].T.reshape(cols, nz, ny, unit).transpose(2, 1, 0, 3)

    pair = jnp.concatenate([w_gate[0], w_up[0]], axis=1)

    slot_ids = jnp.arange(slot_count, dtype=jnp.int32)
    matches = (expert_ids[None, :, :] == (slot_ids // CAP)[:, None, None]) & (
        slots[None, :, :] == (slot_ids % CAP)[:, None, None]
    )
    table = jnp.any(matches, axis=2).astype(jnp.bfloat16)
    outgoing = jnp.dot(table, tokens, preferred_element_type=jnp.float32)
    root = jnp.sqrt(jnp.abs(outgoing * 2.0**29))
    outgoing = jnp.where(outgoing < 0, -root, root).astype(jnp.float16)
    arrived = lax.all_to_all(outgoing, GROUP, split_axis=0, concat_axis=0, tiled=True)
    portion = lax.all_gather(arrived, PLANE, axis=0, tiled=True)
    root = portion.astype(jnp.float32)
    x = (root * jnp.abs(root)).astype(jnp.bfloat16)
    both = jnp.dot(x, pair, preferred_element_type=jnp.float32) * 2.0**-29
    gate, up = both[:, :unit], both[:, unit:]
    hidden = jax.nn.silu(gate) * up
    packed = jnp.sqrt(jnp.sqrt(jnp.abs(hidden * 2.0**40)))
    packed = jnp.where(hidden < 0, -packed, packed).astype(jnp.float16)
    packed, wd = lax.optimization_barrier((packed, wd))
    wd = lax.all_to_all(wd, "y", split_axis=0, concat_axis=0, tiled=True)
    spread = lax.all_gather(packed.reshape(slot_count, -1, unit), "z", axis=0, tiled=True)
    spread = spread.reshape(nz, rows, unit)
    spread = spread.astype(jnp.float32)
    h = (spread * jnp.abs(spread) * (spread * spread * 2.0**-40)).astype(jnp.bfloat16)
    weights = jnp.sum(jnp.where(matches, mix_weights[None, :, :], 0.0), axis=2).astype(jnp.bfloat16)
    h, weights = lax.optimization_barrier((h, weights))
    part = down(h, wd)
    part = part.reshape(nz * ny, slot_count, ny * cols)
    part = lax.all_to_all(part, PLANE, split_axis=0, concat_axis=0, tiled=True)
    part = part.reshape(nz, ny, slot_count, ny * cols).astype(jnp.float32).sum(axis=1)
    result = part.transpose(1, 0, 2).reshape(slot_count, width).astype(jnp.bfloat16)
    back = lax.all_to_all(result, GROUP, split_axis=0, concat_axis=0, tiled=True)
    mixed = jnp.dot(weights.T, back, preferred_element_type=jnp.float32)
    return mixed.astype(jnp.bfloat16)


def solution(mesh):
    experts, dp = mesh.devices.shape
    ny = 8 if dp % 8 == 0 else 1
    split = Mesh(
        mesh.devices.reshape(experts // 2, 2, dp // ny, ny), ("x", "core", "z", "y")
    )
    tok = P(GROUP + PLANE, None)
    weight = P(GROUP, None, PLANE)
    return jax.shard_map(
        shards,
        mesh=split,
        in_specs=(tok, tok, tok, tok, weight, weight, weight),
        out_specs=tok,
        check_vma=False,
    )
```

```python
import jax
import jax.numpy as jnp
from jax import lax
from jax.experimental import pallas as pl
from jax.experimental.pallas import tpu as pltpu
from jax.sharding import Mesh, PartitionSpec as P

CAP = 2
GROUP = ("x", "core")
PLANE = ("z", "y")


def down_kernel(h_ref, w_ref, o_ref, w_all):
    nz, _, unit = h_ref.shape
    ny, _, cols, _ = w_ref.shape
    for z in range(nz):
        for y in range(ny):
            w_all[pl.ds(y * cols, cols), pl.ds(z * unit, unit)] = w_ref[y, z]

    h = jnp.concatenate([h_ref[z] for z in range(nz)], axis=1)
    o_ref[...] = lax.dot_general(
        h, w_all[...], (((1,), (1,)), ((), ())), preferred_element_type=jnp.float32
    ).astype(o_ref.dtype)


def down(h, w):
    nz, rows, unit = h.shape
    ny, _, cols, _ = w.shape
    return pl.pallas_call(
        down_kernel,
        out_shape=jax.ShapeDtypeStruct((rows, ny * cols), jnp.bfloat16),
        in_specs=[pl.BlockSpec(memory_space=pltpu.VMEM)] * 2,
        out_specs=pl.BlockSpec(memory_space=pltpu.VMEM),
        compiler_params=pltpu.CompilerParams(vmem_limit_bytes=20 << 20),
        scratch_shapes=[pltpu.VMEM((ny * cols, nz * unit), jnp.bfloat16)],
        cost_estimate=pl.CostEstimate(
            flops=2 * rows * nz * unit * ny * cols, bytes_accessed=4 << 20, transcendentals=0
        ),
    )(h, w)


def shards(tokens, expert_ids, slots, mix_weights, w_gate, w_up, w_down):
    _, width = tokens.shape
    experts = lax.axis_size(GROUP)
    nz, ny = lax.axis_size("z"), lax.axis_size("y")
    slot_count = experts * CAP
    unit = w_gate.shape[2]
    cols = w_down.shape[2]

    wd = w_down[0].T.reshape(cols, nz, ny, unit).transpose(2, 1, 0, 3)

    pair = jnp.concatenate([w_gate[0], w_up[0]], axis=1)

    slot_ids = jnp.arange(slot_count, dtype=jnp.int32)
    matches = (expert_ids[None, :, :] == (slot_ids // CAP)[:, None, None]) & (
        slots[None, :, :] == (slot_ids % CAP)[:, None, None]
    )
    table = jnp.any(matches, axis=2).astype(jnp.bfloat16)
    outgoing = jnp.dot(table, tokens, preferred_element_type=jnp.float32)
    root = jnp.sqrt(jnp.abs(outgoing * 2.0**29))
    outgoing = jnp.where(outgoing < 0, -root, root).astype(jnp.float16)
    arrived = lax.all_to_all(outgoing, GROUP, split_axis=0, concat_axis=0, tiled=True)
    portion = lax.all_gather(arrived, PLANE, axis=0, tiled=True)
    root = portion.astype(jnp.float32)
    x = (root * jnp.abs(root)).astype(jnp.bfloat16)
    both = jnp.dot(x, pair, preferred_element_type=jnp.float32)
    both, wd = lax.optimization_barrier((both, wd))
    wd = lax.all_to_all(wd, "y", split_axis=0, concat_axis=0, tiled=True)
    both = both * 2.0**-29
    gate, up = both[:, :unit], both[:, unit:]
    hidden = jax.nn.silu(gate) * up
    packed = jnp.sqrt(jnp.sqrt(jnp.abs(hidden * 2.0**40)))
    packed = jnp.where(hidden < 0, -packed, packed).astype(jnp.float16)
    spread = lax.all_gather(packed, "z", axis=0, tiled=False)
    spread = spread.astype(jnp.float32)
    h = (spread * jnp.abs(spread) * (spread * spread * 2.0**-40)).astype(jnp.bfloat16)
    weights = jnp.sum(jnp.where(matches, mix_weights[None, :, :], 0.0), axis=2).astype(jnp.bfloat16)
    h, weights = lax.optimization_barrier((h, weights))
    part = down(h, wd)
    part = part.reshape(nz * ny, slot_count, ny * cols)
    part = lax.all_to_all(part, PLANE, split_axis=0, concat_axis=0, tiled=True)
    part = part.reshape(nz, ny, slot_count, ny * cols).astype(jnp.float32).sum(axis=1)
    result = part.transpose(1, 0, 2).reshape(slot_count, width).astype(jnp.bfloat16)
    back = lax.all_to_all(result, GROUP, split_axis=0, concat_axis=0, tiled=True)
    mixed = jnp.dot(weights.T, back, preferred_element_type=jnp.float32)
    return mixed.astype(jnp.bfloat16)


def solution(mesh):
    experts, dp = mesh.devices.shape
    ny = 8 if dp % 8 == 0 else 1
    split = Mesh(
        mesh.devices.reshape(experts // 2, 2, dp // ny, ny), ("x", "core", "z", "y")
    )
    tok = P(GROUP + PLANE, None)
    weight = P(GROUP, None, PLANE)
    return jax.shard_map(
        shards,
        mesh=split,
        in_specs=(tok, tok, tok, tok, weight, weight, weight),
        out_specs=tok,
        check_vma=False,
    )
```

```python
import jax
import jax.numpy as jnp
from jax import lax
from jax.experimental import pallas as pl
from jax.experimental.pallas import tpu as pltpu
from jax.sharding import Mesh, PartitionSpec as P

CAP = 2
GROUP = ("x", "core")
PLANE = ("z", "y")


def down_kernel(h_ref, w_ref, o_ref):
    h = jnp.concatenate([h_ref[i] for i in range(h_ref.shape[0])], axis=1)
    o_ref[...] = lax.dot_general(
        h, w_ref[...], (((1,), (1,)), ((), ())), preferred_element_type=jnp.float32
    ).astype(o_ref.dtype)


def down(h, w):
    parts, rows, unit = h.shape
    return pl.pallas_call(
        down_kernel,
        out_shape=jax.ShapeDtypeStruct((rows, w.shape[0]), jnp.bfloat16),
        in_specs=[pl.BlockSpec(memory_space=pltpu.VMEM)] * 2,
        out_specs=pl.BlockSpec(memory_space=pltpu.VMEM),
        compiler_params=pltpu.CompilerParams(vmem_limit_bytes=20 << 20),
        cost_estimate=pl.CostEstimate(
            flops=2 * rows * parts * unit * w.shape[0], bytes_accessed=4 << 20, transcendentals=0
        ),
    )(h, w)


def shards(tokens, expert_ids, slots, mix_weights, w_gate, w_up, w_down):
    _, width = tokens.shape
    experts = lax.axis_size(GROUP)
    nz, ny = lax.axis_size("z"), lax.axis_size("y")
    slot_count = experts * CAP
    unit = w_gate.shape[2]
    cols = w_down.shape[2]

    wd = w_down[0].T.reshape(cols, nz, ny, unit).transpose(2, 0, 1, 3)
    wd = wd.reshape(ny, cols, nz * unit)

    pair = jnp.concatenate([w_gate[0], w_up[0]], axis=1)

    slot_ids = jnp.arange(slot_count, dtype=jnp.int32)
    matches = (expert_ids[None, :, :] == (slot_ids // CAP)[:, None, None]) & (
        slots[None, :, :] == (slot_ids % CAP)[:, None, None]
    )
    table = jnp.any(matches, axis=2).astype(jnp.bfloat16)
    outgoing = jnp.dot(table, tokens, preferred_element_type=jnp.float32)
    root = jnp.sqrt(jnp.abs(outgoing * 2.0**29))
    outgoing = jnp.where(outgoing < 0, -root, root).astype(jnp.float16)
    arrived = lax.all_to_all(outgoing, GROUP, split_axis=0, concat_axis=0, tiled=True)
    portion = lax.all_gather(arrived, PLANE, axis=0, tiled=True)
    root = portion.astype(jnp.float32)
    x = (root * jnp.abs(root)).astype(jnp.bfloat16)
    both = jnp.dot(x, pair, preferred_element_type=jnp.float32) * 2.0**-29
    gate, up = both[:, :unit], both[:, unit:]
    hidden = jax.nn.silu(gate) * up
    packed = jnp.sqrt(jnp.sqrt(jnp.abs(hidden * 2.0**40)))
    packed = jnp.where(hidden < 0, -packed, packed).astype(jnp.float16)
    packed, wd = lax.optimization_barrier((packed, wd))
    wd = lax.all_to_all(wd, "y", split_axis=0, concat_axis=0, tiled=True)
    spread = lax.all_gather(packed, "z", axis=0, tiled=False)
    spread = spread.astype(jnp.float32)
    h = (spread * jnp.abs(spread) * (spread * spread * 2.0**-40)).astype(jnp.bfloat16)
    weights = jnp.sum(jnp.where(matches, mix_weights[None, :, :], 0.0), axis=2).astype(jnp.bfloat16)
    h, weights = lax.optimization_barrier((h, weights))
    part = down(h, wd.reshape(ny * cols, nz * unit))
    part = part.reshape(nz * ny, slot_count, ny * cols)
    part = lax.all_to_all(part, PLANE, split_axis=0, concat_axis=0, tiled=True)
    part = part.reshape(nz, ny, slot_count, ny * cols).astype(jnp.float32).sum(axis=1)
    result = part.transpose(1, 0, 2).reshape(slot_count, width).astype(jnp.bfloat16)
    back = lax.all_to_all(result, GROUP, split_axis=0, concat_axis=0, tiled=True)
    mixed = jnp.dot(weights.T, back, preferred_element_type=jnp.float32)
    return mixed.astype(jnp.bfloat16)


def solution(mesh):
    experts, dp = mesh.devices.shape
    ny = 8 if dp % 8 == 0 else 1
    split = Mesh(
        mesh.devices.reshape(experts // 2, 2, dp // ny, ny), ("x", "core", "z", "y")
    )
    tok = P(GROUP + PLANE, None)
    weight = P(GROUP, None, PLANE)
    return jax.shard_map(
        shards,
        mesh=split,
        in_specs=(tok, tok, tok, tok, weight, weight, weight),
        out_specs=tok,
        check_vma=False,
    )
```
